128 devices in a mesh: dp: 1, sp: 128 (over z, y, x, core).
Axes of the slice: x: 4, y: 4, z: 4, core: 2. Of those that a mesh axis runs over, the one named last changes fastest.
Arguments:
- signal: bfloat16 [64, 4096, 512], P('dp', 'sp')
- cond_feats: bfloat16 [64, 4096, 256], P('dp', 'sp')
- w_now: bfloat16 [10, 512, 1024], replicated
- w_past: bfloat16 [10, 512, 1024], replicated
- w_cond: bfloat16 [10, 256, 1024], replicated
- b_gate: float32 [10, 1024], replicated
- w_res: bfloat16 [10, 512, 512], replicated
- w_skip: bfloat16 [10, 512, 256], replicated
Outputs:
- output 1: float32 [64, 4096, 512], P('dp', 'sp')
- output 2: float32 [64, 4096, 256], P('dp', 'sp')
All inputs are finite; a program needn't handle non-finite values.
Results may differ from the reference program's by a relative error of at most 0.00665394.
Values are sent between devices in bfloat16 or wider.
A program may use at most 1 GiB of HBM per device.

```python
import jax
import jax.numpy as jnp

BATCH = 64
SEQ_LEN = 4096
CHANNELS = 512
SKIP_CH = 256
COND_CH = 256
LAYERS = 10


def setup_inputs(seed: int = 0, part: int = 0) -> dict:
    part_key = jax.random.fold_in(jax.random.key(seed), part)
    sig_key, cond_key = jax.random.split(part_key, 2)
    weight_keys = jax.random.split(jax.random.key(seed + 1), 6)
    gate_scale = (2 * CHANNELS + COND_CH) ** -0.5
    out_scale = CHANNELS ** -0.5
    signal = jax.random.normal(sig_key, (BATCH, SEQ_LEN, CHANNELS), jnp.float32)
    cond_feats = jax.random.normal(cond_key, (BATCH, SEQ_LEN, COND_CH), jnp.float32)
    w_now = jax.random.normal(weight_keys[0], (LAYERS, CHANNELS, 2 * CHANNELS), jnp.float32) * gate_scale
    w_past = jax.random.normal(weight_keys[1], (LAYERS, CHANNELS, 2 * CHANNELS), jnp.float32) * gate_scale
    w_cond = jax.random.normal(weight_keys[2], (LAYERS, COND_CH, 2 * CHANNELS), jnp.float32) * gate_scale
    b_gate = 0.5 * jax.random.normal(weight_keys[3], (LAYERS, 2 * CHANNELS), jnp.float32)
    w_res = jax.random.normal(weight_keys[4], (LAYERS, CHANNELS, CHANNELS), jnp.float32) * out_scale
    w_skip = jax.random.normal(weight_keys[5], (LAYERS, CHANNELS, SKIP_CH), jnp.float32) * out_scale
    return {
        'signal': signal.astype(jnp.bfloat16),
        'cond_feats': cond_feats.astype(jnp.bfloat16),
        'w_now': w_now.astype(jnp.bfloat16),
        'w_past': w_past.astype(jnp.bfloat16),
        'w_cond': w_cond.astype(jnp.bfloat16),
        'b_gate': b_gate,
        'w_res': w_res.astype(jnp.bfloat16),
        'w_skip': w_skip.astype(jnp.bfloat16),
    }


def reference(signal, cond_feats, w_now, w_past, w_cond, b_gate, w_res, w_skip):
    resid = signal.astype(jnp.float32)
    skip_sum = jnp.zeros((BATCH, SEQ_LEN, SKIP_CH), jnp.float32)
    cond_wide = cond_feats.astype(jnp.float32)
    for layer in range(LAYERS):
        dilation = 2 ** layer
        now_in = resid.astype(jnp.bfloat16)
        past_in = jnp.concatenate([jnp.zeros((BATCH, dilation, CHANNELS), jnp.bfloat16), now_in[:, :SEQ_LEN - dilation]], axis=1)
        gate_pre = (jnp.einsum('bsc,cg->bsg', now_in.astype(jnp.float32), w_now[layer].astype(jnp.float32))
                    + jnp.einsum('bsc,cg->bsg', past_in.astype(jnp.float32), w_past[layer].astype(jnp.float32))
                    + jnp.einsum('bsc,cg->bsg', cond_wide, w_cond[layer].astype(jnp.float32))
                    + b_gate[layer])
        gated = (jnp.tanh(gate_pre[..., :CHANNELS]) * jax.nn.sigmoid(gate_pre[..., CHANNELS:])).astype(jnp.bfloat16)
        gated_wide = gated.astype(jnp.float32)
        resid = resid + jnp.einsum('bsc,cd->bsd', gated_wide, w_res[layer].astype(jnp.float32))
        skip_sum = skip_sum + jnp.einsum('bsc,cd->bsd', gated_wide, w_skip[layer].astype(jnp.float32))
    return resid, skip_sum
```

```python
import functools

import jax
import jax.numpy as jnp
from jax import lax
from jax.experimental import pallas as pl
from jax.experimental.pallas import tpu as pltpu
from jax.sharding import PartitionSpec as P

LAYERS = 10
NEAR = 5
GROUP = 16
SPAN = 32
ROWS = GROUP * SPAN
HALF = ROWS // 2
FRONT = GROUP * SPAN // 2
CH = 512
COND = 256
SKIP = 256


def kernel(n, chunks, sig, cond, w_now, w_past, w_cond, bias, w_res, w_skip, h_out, s_out,
           wz, wr, ws, h, skip, cnd, ub, edge, far, w_sem, in_sem, out_sem, send_sem, recv_sem):
    me = lax.axis_index('sp')

    def hop(k):
        return 1 if k < NEAR else 2 ** (k - NEAR)

    def parts(k):
        return 1 if k < NEAR else 2

    def weight_copies(k):
        return [pltpu.make_async_copy(w_now.at[k], wz.at[k, pl.ds(0, CH)], w_sem.at[k, 0]),
                pltpu.make_async_copy(w_past.at[k], wz.at[k, pl.ds(CH, CH)], w_sem.at[k, 1]),
                pltpu.make_async_copy(w_cond.at[k], wz.at[k, pl.ds(2 * CH, COND)], w_sem.at[k, 2]),
                pltpu.make_async_copy(w_res.at[k], wr.at[k], w_sem.at[k, 3]),
                pltpu.make_async_copy(w_skip.at[k], ws.at[k], w_sem.at[k, 4])]

    def input_copies(c):
        return [pltpu.make_async_copy(sig.at[c], ub.at[0, c, pl.ds(FRONT, ROWS)], in_sem.at[c, 0]),
                pltpu.make_async_copy(cond.at[c], cnd.at[c], in_sem.at[c, 1])]

    def output_copies(c, half):
        rows = pl.ds(half * HALF, HALF)
        return [pltpu.make_async_copy(h.at[c, rows], h_out.at[c, rows], out_sem.at[c, half, 0]),
                pltpu.make_async_copy(skip.at[c, rows], s_out.at[c, rows], out_sem.at[c, half, 1])]

    def remote(k, c, half):
        if k < NEAR:
            rows = GROUP * 2 ** k
            src = ub.at[k % 2, c, pl.ds(FRONT + ROWS - rows, rows)]
            dst = edge.at[c, pl.ds(rows - GROUP, rows)]
        else:
            src = ub.at[k % 2, c, pl.ds(FRONT + half * HALF, HALF)]
            dst = far.at[k - NEAR, c, pl.ds(half * HALF, HALF)]
        return pltpu.make_async_remote_copy(
            src_ref=src, dst_ref=dst, send_sem=send_sem.at[k, c, half], recv_sem=recv_sem.at[k, c, half],
            device_id={'sp': lax.rem(me + hop(k), n)}, device_id_type=pl.DeviceIdType.MESH)

    def send(k, c, half):
        @pl.when(me + hop(k) < n)
        def _():
            remote(k, c, half).start()

    def wait_sent(k, c, half):
        @pl.when(me + hop(k) < n)
        def _():
            remote(k, c, half).wait_send()

    for copy in input_copies(0):
        copy.start()
    for copy in weight_copies(0):
        copy.start()
    for c in range(1, chunks):
        for copy in input_copies(c):
            copy.start()
    for k in range(1, LAYERS):
        for copy in weight_copies(k):
            copy.start()

    barrier = pltpu.get_barrier_semaphore()
    hops = sorted({hop(k) for k in range(LAYERS)})
    for step in hops:
        for other in (me + step, me + n - step):
            pl.semaphore_signal(barrier, inc=1, device_id={'sp': lax.rem(other, n)},
                                device_id_type=pl.DeviceIdType.MESH)
    pl.semaphore_wait(barrier, 2 * len(hops))

    for c in range(chunks):
        for copy in input_copies(c):
            copy.wait()
        send(0, c, 0)

    def compute(k, c, half):
        rows = pl.ds(half * HALF, HALF)
        own = ub[k % 2, c, pl.ds(FRONT + half * HALF, HALF)]
        if k < NEAR:
            past = ub[k % 2, c, pl.ds(FRONT + half * HALF - GROUP * 2 ** k, HALF)]
        else:
            past = far[k - NEAR, c, rows]
        x = jnp.concatenate([own, past, cnd[c, rows]], axis=1)
        gated = []
        for col in range(0, CH, 256):
            zf = jnp.dot(x, wz[k, :, col:col + 256], preferred_element_type=jnp.float32)
            zg = jnp.dot(x, wz[k, :, CH + col:CH + col + 256], preferred_element_type=jnp.float32)
            zf = zf + bias[k:k + 1, col:col + 256]
            zg = zg + bias[k:k + 1, CH + col:CH + col + 256]
            gated.append((jnp.tanh(zf) * (0.5 * jnp.tanh(0.5 * zg) + 0.5)).astype(jnp.bfloat16))
        a = jnp.concatenate(gated, axis=1)
        for col in range(0, CH, 256):
            cols = pl.ds(col, 256)
            old = own[:, col:col + 256].astype(jnp.float32) if k == 0 else h[c, rows, cols]
            new = old + jnp.dot(a, wr[k, :, col:col + 256], preferred_element_type=jnp.float32)
            h[c, rows, cols] = new
            if k + 1 < LAYERS:
                ub[(k + 1) % 2, c, pl.ds(FRONT + half * HALF, HALF), cols] = new.astype(jnp.bfloat16)
        add = jnp.dot(a, ws[k], preferred_element_type=jnp.float32)
        skip[c, rows] = add if k == 0 else skip[c, rows] + add

    def receive(k, c, half):
        if k < NEAR:
            rows = GROUP * 2 ** k
            front = pl.ds(FRONT - rows, rows)

            @pl.when(me >= hop(k))
            def _():
                remote(k, c, half).wait_recv()
                ub[k % 2, c, front] = edge[c, pl.ds(rows - GROUP, rows)]

            @pl.when(me < hop(k))
            def _():
                ub[k % 2, c, front] = jnp.zeros((rows, CH), jnp.bfloat16)
        else:
            @pl.when(me >= hop(k))
            def _():
                remote(k, c, half).wait_recv()

            @pl.when(me < hop(k))
            def _():
                far[k - NEAR, c, pl.ds(half * HALF, HALF)] = jnp.zeros((HALF, CH), jnp.bfloat16)

    def task(k, c):
        @pl.when(c == 0)
        def _():
            for copy in weight_copies(k):
                copy.wait()

        for half in (1, 0):
            if k >= NEAR or half == 0:
                receive(k, c, half if k >= NEAR else 0)
            if 1 <= k < LAYERS - 1:
                if k - 1 >= NEAR:
                    wait_sent(k - 1, c, half)
                elif half == 1:
                    wait_sent(k - 1, c, 0)
            compute(k, c, half)
            if k + 1 == LAYERS:
                for copy in output_copies(c, half):
                    copy.start()
            elif k + 1 >= NEAR:
                send(k + 1, c, half)
            elif half == 1:
                send(k + 1, c, 0)

    def wave(w, carry):
        for k in reversed(range(LAYERS)):
            c = w - k

            @pl.when((c >= 0) & (c < chunks))
            def _():
                task(k, c)
        return carry

    lax.fori_loop(0, LAYERS + chunks - 1, wave, 0)

    def finish(c, carry):
        for half in (1, 0):
            for k in (LAYERS - 2, LAYERS - 1):
                wait_sent(k, c, half)
            for copy in output_copies(c, half):
                copy.wait()
        return carry

    lax.fori_loop(0, chunks, finish, 0)


def solution(mesh):
    n = mesh.shape['sp']

    def local(signal, cond_feats, w_now, w_past, w_cond, b_gate, w_res, w_skip):
        batch = signal.shape[0]
        chunks = batch // GROUP

        def pack(v):
            v = v.reshape(chunks, GROUP, SPAN, v.shape[2])
            return v.transpose(0, 2, 1, 3).reshape(chunks, ROWS, v.shape[3])

        def unpack(v):
            v = v.reshape(chunks, SPAN, GROUP, v.shape[2])
            return v.transpose(0, 2, 1, 3).reshape(batch, SPAN, v.shape[3])

        hbm = pl.BlockSpec(memory_space=pl.ANY)
        h, s = pl.pallas_call(
            functools.partial(kernel, n, chunks),
            out_shape=(jax.ShapeDtypeStruct((chunks, ROWS, CH), jnp.float32),
                       jax.ShapeDtypeStruct((chunks, ROWS, SKIP), jnp.float32)),
            in_specs=[hbm] * 5 + [pl.BlockSpec(memory_space=pltpu.VMEM)] + [hbm] * 2,
            out_specs=(hbm, hbm),
            scratch_shapes=[
                pltpu.VMEM((LAYERS, 2 * CH + COND, 2 * CH), jnp.bfloat16),
                pltpu.VMEM((LAYERS, CH, CH), jnp.bfloat16),
                pltpu.VMEM((LAYERS, CH, SKIP), jnp.bfloat16),
                pltpu.VMEM((chunks, ROWS, CH), jnp.float32),
                pltpu.VMEM((chunks, ROWS, SKIP), jnp.float32),
                pltpu.VMEM((chunks, ROWS, COND), jnp.bfloat16),
                pltpu.VMEM((2, chunks, FRONT + ROWS, CH), jnp.bfloat16),
                pltpu.VMEM((chunks, GROUP * (SPAN - 1), CH), jnp.bfloat16),
                pltpu.VMEM((LAYERS - NEAR, chunks, ROWS, CH), jnp.bfloat16),
                pltpu.SemaphoreType.DMA((LAYERS, 5)),
                pltpu.SemaphoreType.DMA((chunks, 2)),
                pltpu.SemaphoreType.DMA((chunks, 2, 2)),
                pltpu.SemaphoreType.DMA((LAYERS, chunks, 2)),
                pltpu.SemaphoreType.DMA((LAYERS, chunks, 2)),
            ],
            compiler_params=pltpu.CompilerParams(
                collective_id=0, has_side_effects=True, vmem_limit_bytes=67043328),
        )(pack(signal), pack(cond_feats), w_now, w_past, w_cond, b_gate, w_res, w_skip)
        return unpack(h), unpack(s)

    seq = P('dp', 'sp', None)
    return jax.shard_map(local, mesh=mesh, in_specs=(seq, seq, P(), P(), P(), P(), P(), P()),
                         out_specs=(seq, seq), check_vma=False)
```

```python
import functools

import jax
import jax.numpy as jnp
from jax import lax
from jax.experimental import pallas as pl
from jax.experimental.pallas import tpu as pltpu
from jax.sharding import PartitionSpec as P

LAYERS = 10
NEAR = 5
RING = 8
BLOCKS = 16
CHUNKS = 4
SPAN = 32
ROWS = BLOCKS * SPAN
HALF = ROWS // 2
PAD = 2 * SPAN
CH = 512
COND = 256
SKIP = 256
MESH = pl.DeviceIdType.MESH


def kernel(sig, cond, w_now, w_past, w_cond, bias, w_res, w_skip, h_out, s_out,
           wz, wr, ws, h, skip, cnd, ub, far, shifted, edge_out, edge_in,
           w_sem, own_sem, in_send, in_recv, edge_send, edge_recv, far_send, far_recv, out_send, out_recv, out_own):
    me = lax.axis_index('sp')
    row, lane = me // RING, lax.rem(me, RING)

    def ring(step):
        return {'sp': row * RING + lax.rem(lane + step, RING)}

    def peer(step):
        return lax.rem(row + step, BLOCKS)

    def hop(k):
        return 1 if k <= NEAR else 2 ** (k - NEAR)

    def weight_copies(k):
        return [pltpu.make_async_copy(w_now.at[k], wz.at[k, pl.ds(0, CH)], w_sem.at[k, 0]),
                pltpu.make_async_copy(w_past.at[k], wz.at[k, pl.ds(CH, CH)], w_sem.at[k, 1]),
                pltpu.make_async_copy(w_cond.at[k], wz.at[k, pl.ds(2 * CH, COND)], w_sem.at[k, 2]),
                pltpu.make_async_copy(w_res.at[k], wr.at[k], w_sem.at[k, 3]),
                pltpu.make_async_copy(w_skip.at[k], ws.at[k], w_sem.at[k, 4])]

    def block(b, start=0):
        return pl.ds(pl.multiple_of(start + b * SPAN, SPAN), SPAN)

    def own_inputs(c):
        seq = row * CHUNKS + c
        return [pltpu.make_async_copy(sig.at[seq], ub.at[0, c, block(row, PAD)], own_sem.at[c, 0]),
                pltpu.make_async_copy(cond.at[seq], cnd.at[c, block(row)], own_sem.at[c, 1])]

    def peer_inputs(c, step):
        to = peer(step)
        seq = to * CHUNKS + c
        dev = {'sp': to * RING + lane}
        return [pltpu.make_async_remote_copy(sig.at[seq], ub.at[0, c, block(row, PAD)], in_send.at[c, 0],
                                             in_recv.at[c, 0], device_id=dev, device_id_type=MESH),
                pltpu.make_async_remote_copy(cond.at[seq], cnd.at[c, block(row)], in_send.at[c, 1],
                                             in_recv.at[c, 1], device_id=dev, device_id_type=MESH)]

    def all_inputs(c):
        others = pl.ds(0, ROWS - SPAN)
        return [pltpu.make_async_remote_copy(ub.at[0, c, others], ub.at[0, c, others], in_send.at[c, 0],
                                             in_recv.at[c, 0], device_id=ring(1), device_id_type=MESH),
                pltpu.make_async_remote_copy(cnd.at[c, others], cnd.at[c, others], in_send.at[c, 1],
                                             in_recv.at[c, 1], device_id=ring(1), device_id_type=MESH)]

    def own_outputs(c):
        seq = row * CHUNKS + c
        return [pltpu.make_async_copy(h.at[c, block(row)], h_out.at[seq], out_own.at[c, 0]),
                pltpu.make_async_copy(skip.at[c, block(row)], s_out.at[seq], out_own.at[c, 1])]

    def peer_outputs(c, step):
        to = peer(step)
        seq = row * CHUNKS + c
        dev = {'sp': to * RING + lane}
        return [pltpu.make_async_remote_copy(h.at[c, block(to)], h_out.at[seq], out_send.at[c, 0],
                                             out_recv.at[c, 0], device_id=dev, device_id_type=MESH),
                pltpu.make_async_remote_copy(skip.at[c, block(to)], s_out.at[seq], out_send.at[c, 1],
                                             out_recv.at[c, 1], device_id=dev, device_id_type=MESH)]

    def all_outputs(c):
        others = pl.ds(0, BLOCKS - 1)
        return [pltpu.make_async_remote_copy(h_out.at[others], h_out.at[others], out_send.at[c, 0],
                                             out_recv.at[c, 0], device_id=ring(1), device_id_type=MESH),
                pltpu.make_async_remote_copy(s_out.at[others], s_out.at[others], out_send.at[c, 1],
                                             out_recv.at[c, 1], device_id=ring(1), device_id_type=MESH)]

    def edge_copy(k, c):
        rows = pl.ds(BLOCKS * (2 ** k - 1), BLOCKS * 2 ** k)
        return pltpu.make_async_remote_copy(edge_out.at[c, rows], edge_in.at[c, rows], edge_send.at[k, c],
                                            edge_recv.at[k, c], device_id=ring(1), device_id_type=MESH)

    def far_copy(k, c, half):
        return pltpu.make_async_remote_copy(
            ub.at[k % 2, c, pl.ds(PAD + half * HALF, HALF)], far.at[k - NEAR, c, pl.ds(SPAN + half * HALF, HALF)],
            far_send.at[k - NEAR, c, half], far_recv.at[k - NEAR, c, half], device_id=ring(hop(k)), device_id_type=MESH)

    for c in range(CHUNKS):
        for copy in own_inputs(c):
            copy.start()
    for copy in weight_copies(0):
        copy.start()

    barrier = pltpu.get_barrier_semaphore()
    ring_steps = (1, 2, 4, RING - 2, RING - 1)
    for step in ring_steps:
        pl.semaphore_signal(barrier, inc=1, device_id=ring(step), device_id_type=MESH)
    for step in range(1, BLOCKS):
        pl.semaphore_signal(barrier, inc=1, device_id={'sp': peer(step) * RING + lane}, device_id_type=MESH)
    pl.semaphore_wait(barrier, len(ring_steps) + BLOCKS - 1)

    def start_inputs(i, carry):
        c, step = i // (BLOCKS - 1), lax.rem(i, BLOCKS - 1) + 1
        for copy in peer_inputs(c, step):
            copy.start()
        return carry

    lax.fori_loop(0, CHUNKS * (BLOCKS - 1), start_inputs, 0)
    for k in range(1, LAYERS):
        for copy in weight_copies(k):
            copy.start()

    for c in range(CHUNKS):
        for parity in range(2):
            ub[parity, c, pl.ds(0, PAD)] = jnp.zeros((PAD, CH), jnp.bfloat16)
        for k in range(far.shape[0]):
            far[k, c, pl.ds(0, SPAN)] = jnp.zeros((SPAN, CH), jnp.bfloat16)

    lanes = range(CH // 128)

    def send_edges(k, c):
        d = 2 ** k

        def roll(b, carry):
            for t in lanes:
                shifted[c, t, block(b)] = pltpu.roll(h[c, block(b), pl.ds(128 * t, 128)], d, 0)
            return carry

        lax.fori_loop(0, BLOCKS, roll, 0)
        for j in range(d):
            for t in lanes:
                rows = shifted[c, t, pl.ds(j, BLOCKS, stride=SPAN), :]
                edge_out[c, pl.ds(BLOCKS * (d - 1 + j), BLOCKS), pl.ds(128 * t, 128)] = rows.astype(jnp.bfloat16)
        edge_copy(k, c).start()

    def arrive(c):
        for copy in own_inputs(c):
            copy.wait()
        for copy in all_inputs(c):
            copy.wait_recv()
        h[c] = ub[0, c, pl.ds(PAD, ROWS)].astype(jnp.float32)
        send_edges(0, c)

    def receive_edges(k, c):
        d = 2 ** k
        edge_copy(k, c).wait_recv()

        def patch(start):
            for j in range(d):
                for t in lanes:
                    rows = edge_in[c, pl.ds(BLOCKS * (d - 1 + j), BLOCKS), pl.ds(128 * t, 128)]
                    shifted[c, t, pl.ds(start + j, BLOCKS, stride=SPAN), :] = rows.astype(jnp.float32)

        @pl.when(lane > 0)
        def _():
            patch(0)

        @pl.when(lane == 0)
        def _():
            patch(SPAN)
            for t in lanes:
                shifted[c, t, pl.ds(0, d)] = jnp.zeros((d, 128), jnp.float32)

    def compute(k, c, half):
        rows = pl.ds(half * HALF, HALF)
        own = ub[k % 2, c, pl.ds(PAD + half * HALF, HALF)]
        if k < NEAR:
            past = jnp.concatenate([shifted[c, t, rows].astype(jnp.bfloat16) for t in lanes], axis=1)
        elif k < far.shape[0] + NEAR:
            wrapped = (lane < hop(k)).astype(jnp.int32)
            start = pl.multiple_of(SPAN - SPAN * wrapped + half * HALF, SPAN)
            past = far[k - NEAR, c, pl.ds(start, HALF)]
        else:
            past = ub[k % 2, c, pl.ds(PAD - SPAN * (k - 7) + half * HALF, HALF)]
        x = jnp.concatenate([own, past, cnd[c, rows]], axis=1)
        gated = []
        for col in range(0, CH, 256):
            zf = jnp.dot(x, wz[k, :, col:col + 256], preferred_element_type=jnp.float32)
            zg = jnp.dot(x, wz[k, :, CH + col:CH + col + 256], preferred_element_type=jnp.float32)
            zf = zf + bias[k:k + 1, col:col + 256]
            zg = zg + bias[k:k + 1, CH + col:CH + col + 256]
            gated.append((jnp.tanh(zf) * (0.5 * jnp.tanh(0.5 * zg) + 0.5)).astype(jnp.bfloat16))
        a = jnp.concatenate(gated, axis=1)
        for col in range(0, CH, 256):
            cols = pl.ds(col, 256)
            new = h[c, rows, cols] + jnp.dot(a, wr[k, :, col:col + 256], preferred_element_type=jnp.float32)
            h[c, rows, cols] = new
            if k + 1 < LAYERS:
                ub[(k + 1) % 2, c, pl.ds(PAD + half * HALF, HALF), cols] = new.astype(jnp.bfloat16)
        add = jnp.dot(a, ws[k], preferred_element_type=jnp.float32)
        skip[c, rows] = add if k == 0 else skip[c, rows] + add

    def task(k, c):
        @pl.when(c == 0)
        def _():
            for copy in weight_copies(k):
                copy.wait()

        if k == 0:
            arrive(c)
        if k < NEAR:
            receive_edges(k, c)
        for half in (0, 1):
            if NEAR <= k < NEAR + far.shape[0]:
                far_copy(k, c, half).wait_recv()
            if NEAR <= k - 1 < NEAR + far.shape[0]:
                far_copy(k - 1, c, half).wait_send()
            compute(k, c, half)
            if NEAR <= k + 1 < NEAR + far.shape[0]:
                far_copy(k + 1, c, half).start()
        if k + 1 < NEAR:
            send_edges(k + 1, c)
        if k + 1 == LAYERS:
            for copy in own_outputs(c):
                copy.start()

            def start_outputs(i, carry):
                for copy in peer_outputs(c, i + 1):
                    copy.start()
                return carry

            lax.fori_loop(0, BLOCKS - 1, start_outputs, 0)

    def wave(w, carry):
        for k in reversed(range(LAYERS)):
            c = w - k

            @pl.when((c >= 0) & (c < CHUNKS))
            def _():
                task(k, c)
        return carry

    lax.fori_loop(0, LAYERS + CHUNKS - 1, wave, 0)

    def finish(c, carry):
        for copy in all_inputs(c):
            copy.wait_send()
        for k in range(NEAR):
            edge_copy(k, c).wait_send()
        for copy in own_outputs(c):
            copy.wait()
        for copy in all_outputs(c):
            copy.wait_send()
            copy.wait_recv()
        return carry

    lax.fori_loop(0, CHUNKS, finish, 0)


def solution(mesh):
    def local(signal, cond_feats, w_now, w_past, w_cond, b_gate, w_res, w_skip):
        hbm = pl.BlockSpec(memory_space=pl.ANY)
        dma = pltpu.SemaphoreType.DMA
        return pl.pallas_call(
            kernel,
            out_shape=(jax.ShapeDtypeStruct(signal.shape, jnp.float32),
                       jax.ShapeDtypeStruct(signal.shape[:2] + (SKIP,), jnp.float32)),
            in_specs=[hbm] * 5 + [pl.BlockSpec(memory_space=pltpu.VMEM)] + [hbm] * 2,
            out_specs=(hbm, hbm),
            scratch_shapes=[
                pltpu.VMEM((LAYERS, 2 * CH + COND, 2 * CH), jnp.bfloat16),
                pltpu.VMEM((LAYERS, CH, CH), jnp.bfloat16),
                pltpu.VMEM((LAYERS, CH, SKIP), jnp.bfloat16),
                pltpu.VMEM((CHUNKS, ROWS, CH), jnp.float32),
                pltpu.VMEM((CHUNKS, ROWS, SKIP), jnp.float32),
                pltpu.VMEM((CHUNKS, ROWS, COND), jnp.bfloat16),
                pltpu.VMEM((2, CHUNKS, PAD + ROWS, CH), jnp.bfloat16),
                pltpu.VMEM((3, CHUNKS, SPAN + ROWS, CH), jnp.bfloat16),
                pltpu.VMEM((CHUNKS, CH // 128, SPAN + ROWS, 128), jnp.float32),
                pltpu.VMEM((CHUNKS, BLOCKS * (SPAN - 1), CH), jnp.bfloat16),
                pltpu.VMEM((CHUNKS, BLOCKS * (SPAN - 1), CH), jnp.bfloat16),
                dma((LAYERS, 5)), dma((CHUNKS, 2)), dma((CHUNKS, 2)), dma((CHUNKS, 2)),
                dma((NEAR, CHUNKS)), dma((NEAR, CHUNKS)), dma((3, CHUNKS, 2)), dma((3, CHUNKS, 2)),
                dma((CHUNKS, 2)), dma((CHUNKS, 2)), dma((CHUNKS, 2)),
            ],
            compiler_params=pltpu.CompilerParams(
                collective_id=0, has_side_effects=True, vmem_limit_bytes=67043328),
        )(signal, cond_feats, w_now, w_past, w_cond, b_gate, w_res, w_skip)

    seq = P('dp', 'sp', None)
    return jax.shard_map(local, mesh=mesh, in_specs=(seq, seq, P(), P(), P(), P(), P(), P()),
                         out_specs=(seq, seq), check_vma=False)
```

```python
import functools

import jax
import jax.numpy as jnp
from jax import lax
from jax.experimental import pallas as pl
from jax.experimental.pallas import tpu as pltpu
from jax.sharding import PartitionSpec as P

LAYERS = 10
NEAR = 5
RING = 8
BLOCKS = 16
CHUNKS = 4
SPAN = 32
ROWS = BLOCKS * SPAN
HALF = ROWS // 2
PAD = 2 * SPAN
RELAYED = 7
SLOT_ARRIVE = 0
SLOTS = (6, 13, 18, 25, 31, 36, 41, 53, 54, 55)
SLOT_FORWARD = 46
SKEW = 11
LAG = 3
CH = 512
COND = 256
SKIP = 256
MESH = pl.DeviceIdType.MESH


def kernel(sig, cond, w_now, w_past, w_cond, bias, w_res, w_skip, h_out, s_out,
           wz, wr, ws, h, skip, cnd, ub, far, relay, shifted, edge_out, edge_in,
           w_sem, own_sem, in_send, in_recv, edge_send, edge_recv, far_send, far_recv, relay_send, relay_recv, out_send, out_recv, out_own):
    me = lax.axis_index('sp')
    row, lane = me // RING, lax.rem(me, RING)

    def ring(step):
        return {'sp': row * RING + lax.rem(lane + step, RING)}

    def peer(step):
        return lax.rem(row + step, BLOCKS)

    def hop(k):
        return 1 if k <= NEAR else 2 ** (k - NEAR)

    def weight_copies(k):
        return [pltpu.make_async_copy(w_now.at[k], wz.at[k, pl.ds(0, CH)], w_sem.at[k, 0]),
                pltpu.make_async_copy(w_past.at[k], wz.at[k, pl.ds(CH, CH)], w_sem.at[k, 1]),
                pltpu.make_async_copy(w_cond.at[k], wz.at[k, pl.ds(2 * CH, COND)], w_sem.at[k, 2]),
                pltpu.make_async_copy(w_res.at[k], wr.at[k], w_sem.at[k, 3]),
                pltpu.make_async_copy(w_skip.at[k], ws.at[k], w_sem.at[k, 4])]

    def block(b, start=0):
        return pl.ds(pl.multiple_of(start + b * SPAN, SPAN), SPAN)

    def own_inputs(c):
        seq = row * CHUNKS + c
        return [pltpu.make_async_copy(sig.at[seq], ub.at[0, c, block(row, PAD)], own_sem.at[c, 0]),
                pltpu.make_async_copy(cond.at[seq], cnd.at[c, block(row)], own_sem.at[c, 1])]

    def peer_inputs(c, step):
        to = peer(step)
        seq = to * CHUNKS + c
        dev = {'sp': to * RING + lane}
        return [pltpu.make_async_remote_copy(sig.at[seq], ub.at[0, c, block(row, PAD)], in_send.at[c, 0],
                                             in_recv.at[c, 0], device_id=dev, device_id_type=MESH),
                pltpu.make_async_remote_copy(cond.at[seq], cnd.at[c, block(row)], in_send.at[c, 1],
                                             in_recv.at[c, 1], device_id=dev, device_id_type=MESH)]

    def all_inputs(c):
        others = pl.ds(0, ROWS - SPAN)
        return [pltpu.make_async_remote_copy(ub.at[0, c, others], ub.at[0, c, others], in_send.at[c, 0],
                                             in_recv.at[c, 0], device_id=ring(1), device_id_type=MESH),
                pltpu.make_async_remote_copy(cnd.at[c, others], cnd.at[c, others], in_send.at[c, 1],
                                             in_recv.at[c, 1], device_id=ring(1), device_id_type=MESH)]

    def own_outputs(c):
        seq = row * CHUNKS + c
        return [pltpu.make_async_copy(h.at[c, block(row)], h_out.at[seq], out_own.at[c, 0]),
                pltpu.make_async_copy(skip.at[c, block(row)], s_out.at[seq], out_own.at[c, 1])]

    def peer_outputs(c, to):
        seq = row * CHUNKS + c
        dev = {'sp': to * RING + lane}
        return [pltpu.make_async_remote_copy(h.at[c, block(to)], h_out.at[seq], out_send.at[c, 0],
                                             out_recv.at[c, 0], device_id=dev, device_id_type=MESH),
                pltpu.make_async_remote_copy(skip.at[c, block(to)], s_out.at[seq], out_send.at[c, 1],
                                             out_recv.at[c, 1], device_id=dev, device_id_type=MESH)]

    def all_outputs(c):
        others = pl.ds(0, BLOCKS - 1)
        return [pltpu.make_async_remote_copy(h_out.at[others], h_out.at[others], out_send.at[c, 0],
                                             out_recv.at[c, 0], device_id=ring(1), device_id_type=MESH),
                pltpu.make_async_remote_copy(s_out.at[others], s_out.at[others], out_send.at[c, 1],
                                             out_recv.at[c, 1], device_id=ring(1), device_id_type=MESH)]

    def edge_copy(k, c):
        rows = pl.ds(BLOCKS * (2 ** k - 1), BLOCKS * 2 ** k)
        return pltpu.make_async_remote_copy(edge_out.at[c, rows], edge_in.at[c, rows], edge_send.at[k, c],
                                            edge_recv.at[k, c], device_id=ring(1), device_id_type=MESH)

    def far_copy(k, c, half):
        rows = pl.ds(half * HALF, HALF)
        src = relay.at[c, rows] if k == RELAYED else ub.at[k % 2, c, pl.ds(PAD + half * HALF, HALF)]
        return pltpu.make_async_remote_copy(
            src, far.at[k - NEAR, c, pl.ds(SPAN + half * HALF, HALF)], far_send.at[k - NEAR, c, half],
            far_recv.at[k - NEAR, c, half], device_id=ring(RING - 2 if k == RELAYED else hop(k)), device_id_type=MESH)

    def relay_copy(c, half):
        return pltpu.make_async_remote_copy(
            ub.at[RELAYED % 2, c, pl.ds(PAD + half * HALF, HALF)], relay.at[c, pl.ds(half * HALF, HALF)],
            relay_send.at[c, half], relay_recv.at[c, half], device_id=ring(RING - 2), device_id_type=MESH)

    def send_far(k, c, half):
        (relay_copy(c, half) if k == RELAYED else far_copy(k, c, half)).start()

    def wait_sent(k, c, half):
        (relay_copy(c, half) if k == RELAYED else far_copy(k, c, half)).wait_send()

    for c in range(CHUNKS):
        for copy in own_inputs(c):
            copy.start()
    for copy in weight_copies(0):
        copy.start()

    barrier = pltpu.get_barrier_semaphore()
    ring_steps = (1, 2, RING - 2, RING - 1)
    for step in ring_steps:
        pl.semaphore_signal(barrier, inc=1, device_id=ring(step), device_id_type=MESH)
    for step in range(1, BLOCKS):
        pl.semaphore_signal(barrier, inc=1, device_id={'sp': peer(step) * RING + lane}, device_id_type=MESH)
    pl.semaphore_wait(barrier, len(ring_steps) + BLOCKS - 1)

    def start_inputs(i, carry):
        c, step = i // (BLOCKS - 1), lax.rem(i, BLOCKS - 1) + 1
        for copy in peer_inputs(c, step):
            copy.start()
        return carry

    lax.fori_loop(0, CHUNKS * (BLOCKS - 1), start_inputs, 0)
    for k in range(1, LAYERS):
        for copy in weight_copies(k):
            copy.start()

    for c in range(CHUNKS):
        for parity in range(2):
            ub[parity, c, pl.ds(0, PAD)] = jnp.zeros((PAD, CH), jnp.bfloat16)
        for k in range(far.shape[0]):
            far[k, c, pl.ds(0, SPAN)] = jnp.zeros((SPAN, CH), jnp.bfloat16)

    lanes = range(CH // 128)

    def send_edges(k, c):
        d = 2 ** k

        def roll(b, carry):
            for t in lanes:
                shifted[c, t, block(b)] = pltpu.roll(h[c, block(b), pl.ds(128 * t, 128)], d, 0)
            return carry

        lax.fori_loop(0, BLOCKS, roll, 0)
        for j in range(d):
            for t in lanes:
                rows = shifted[c, t, pl.ds(j, BLOCKS, stride=SPAN), :]
                edge_out[c, pl.ds(BLOCKS * (d - 1 + j), BLOCKS), pl.ds(128 * t, 128)] = rows.astype(jnp.bfloat16)
        edge_copy(k, c).start()

    def arrive(c):
        for copy in own_inputs(c):
            copy.wait()
        for copy in all_inputs(c):
            copy.wait_recv()
        h[c] = ub[0, c, pl.ds(PAD, ROWS)].astype(jnp.float32)
        send_edges(0, c)

    def receive_edges(k, c):
        d = 2 ** k
        edge_copy(k, c).wait_recv()

        def patch(start):
            for j in range(d):
                for t in lanes:
                    rows = edge_in[c, pl.ds(BLOCKS * (d - 1 + j), BLOCKS), pl.ds(128 * t, 128)]
                    shifted[c, t, pl.ds(start + j, BLOCKS, stride=SPAN), :] = rows.astype(jnp.float32)

        @pl.when(lane > 0)
        def _():
            patch(0)

        @pl.when(lane == 0)
        def _():
            patch(SPAN)
            for t in lanes:
                shifted[c, t, pl.ds(0, d)] = jnp.zeros((d, 128), jnp.float32)

    def compute(k, c, first, count):
        rows = pl.ds(first, count)
        own = ub[k % 2, c, pl.ds(PAD + first, count)]
        if k < NEAR:
            past = jnp.concatenate([shifted[c, t, rows].astype(jnp.bfloat16) for t in lanes], axis=1)
        elif k < far.shape[0] + NEAR:
            wrapped = (lane < hop(k)).astype(jnp.int32)
            start = pl.multiple_of(SPAN - SPAN * wrapped + first, SPAN)
            past = far[k - NEAR, c, pl.ds(start, count)]
        else:
            past = ub[k % 2, c, pl.ds(PAD - SPAN * (k - RELAYED) + first, count)]
        x = jnp.concatenate([own, past, cnd[c, rows]], axis=1)
        gated = []
        for col in range(0, CH, 256):
            zf = jnp.dot(x, wz[k, :, col:col + 256], preferred_element_type=jnp.float32)
            zg = jnp.dot(x, wz[k, :, CH + col:CH + col + 256], preferred_element_type=jnp.float32)
            zf = zf + bias[k:k + 1, col:col + 256]
            zg = zg + bias[k:k + 1, CH + col:CH + col + 256]
            gated.append((jnp.tanh(zf) * (0.5 * jnp.tanh(0.5 * zg) + 0.5)).astype(jnp.bfloat16))
        a = jnp.concatenate(gated, axis=1)
        for col in range(0, CH, 256):
            cols = pl.ds(col, 256)
            new = h[c, rows, cols] + jnp.dot(a, wr[k, :, col:col + 256], preferred_element_type=jnp.float32)
            h[c, rows, cols] = new
            if k + 1 < LAYERS:
                ub[(k + 1) % 2, c, pl.ds(PAD + first, count), cols] = new.astype(jnp.bfloat16)
        add = jnp.dot(a, ws[k], preferred_element_type=jnp.float32)
        skip[c, rows] = add if k == 0 else skip[c, rows] + add

    def near_layer(k, c):
        @pl.when(c == 0)
        def _():
            for copy in weight_copies(k):
                copy.wait()

        receive_edges(k, c)
        compute(k, c, 0, ROWS)
        if k + 1 < NEAR:
            send_edges(k + 1, c)
        else:
            for half in range(2):
                send_far(NEAR, c, half)

    def far_layer(k, half, c):
        if half == 0:
            @pl.when(c == 0)
            def _():
                for copy in weight_copies(k):
                    copy.wait()

        if k <= RELAYED:
            far_copy(k, c, half).wait_recv()
        if NEAR <= k - 1 <= RELAYED:
            wait_sent(k - 1, c, half)
        compute(k, c, half * HALF, HALF)
        if k < RELAYED:
            send_far(k + 1, c, half)
        if k + 1 == LAYERS:
            blocks = BLOCKS // 2

            @pl.when(row // blocks == half)
            def _():
                for copy in own_outputs(c):
                    copy.start()

            def start_outputs(i, carry):
                to = half * blocks + lax.rem(row + i, blocks)

                @pl.when(to != row)
                def _():
                    for copy in peer_outputs(c, to):
                        copy.start()
                return carry

            lax.fori_loop(0, blocks, start_outputs, 0)

    def forward(half, c):
        relay_copy(c, half).wait_recv()
        far_copy(RELAYED, c, half).start()

    steps = [(SLOT_ARRIVE, -1, arrive)]
    for k in range(NEAR):
        steps.append((SLOTS[k], k, functools.partial(near_layer, k)))
    for half in range(2):
        steps.append((SLOT_FORWARD + LAG * half, RELAYED - 0.5 - half / 10, functools.partial(forward, half)))
        for k in range(NEAR, LAYERS):
            steps.append((SLOTS[k] + LAG * half, k - half / 10, functools.partial(far_layer, k, half)))
    steps.sort(key=lambda step: -step[1])

    def wave(w, carry):
        for first, _, step in steps:
            since = w - first + CHUNKS * SKEW
            c = since // SKEW - CHUNKS

            @pl.when((since >= CHUNKS * SKEW) & (lax.rem(since, SKEW) == 0) & (c < CHUNKS))
            def _(step=step, c=c):
                step(c)
        return carry

    waves = max(first for first, _, _ in steps) + SKEW * (CHUNKS - 1) + 1
    lax.fori_loop(0, waves, wave, 0)

    def finish(c, carry):
        for copy in all_inputs(c):
            copy.wait_send()
        for k in range(NEAR):
            edge_copy(k, c).wait_send()
        for half in range(2):
            far_copy(RELAYED, c, half).wait_send()
        for copy in own_outputs(c):
            copy.wait()
        for copy in all_outputs(c):
            copy.wait_send()
            copy.wait_recv()
        return carry

    lax.fori_loop(0, CHUNKS, finish, 0)


def solution(mesh):
    def local(signal, cond_feats, w_now, w_past, w_cond, b_gate, w_res, w_skip):
        hbm = pl.BlockSpec(memory_space=pl.ANY)
        dma = pltpu.SemaphoreType.DMA
        return pl.pallas_call(
            kernel,
            out_shape=(jax.ShapeDtypeStruct(signal.shape, jnp.float32),
                       jax.ShapeDtypeStruct(signal.shape[:2] + (SKIP,), jnp.float32)),
            in_specs=[hbm] * 5 + [pl.BlockSpec(memory_space=pltpu.VMEM)] + [hbm] * 2,
            out_specs=(hbm, hbm),
            scratch_shapes=[
                pltpu.VMEM((LAYERS, 2 * CH + COND, 2 * CH), jnp.bfloat16),
                pltpu.VMEM((LAYERS, CH, CH), jnp.bfloat16),
                pltpu.VMEM((LAYERS, CH, SKIP), jnp.bfloat16),
                pltpu.VMEM((CHUNKS, ROWS, CH), jnp.float32),
                pltpu.VMEM((CHUNKS, ROWS, SKIP), jnp.float32),
                pltpu.VMEM((CHUNKS, ROWS, COND), jnp.bfloat16),
                pltpu.VMEM((2, CHUNKS, PAD + ROWS, CH), jnp.bfloat16),
                pltpu.VMEM((3, CHUNKS, SPAN + ROWS, CH), jnp.bfloat16),
                pltpu.VMEM((CHUNKS, ROWS, CH), jnp.bfloat16),
                pltpu.VMEM((CHUNKS, CH // 128, SPAN + ROWS, 128), jnp.float32),
                pltpu.VMEM((CHUNKS, BLOCKS * (SPAN - 1), CH), jnp.bfloat16),
                pltpu.VMEM((CHUNKS, BLOCKS * (SPAN - 1), CH), jnp.bfloat16),
                dma((LAYERS, 5)), dma((CHUNKS, 2)), dma((CHUNKS, 2)), dma((CHUNKS, 2)),
                dma((NEAR, CHUNKS)), dma((NEAR, CHUNKS)), dma((3, CHUNKS, 2)), dma((3, CHUNKS, 2)),
                dma((CHUNKS, 2)), dma((CHUNKS, 2)),
                dma((CHUNKS, 2)), dma((CHUNKS, 2)), dma((CHUNKS, 2)),
            ],
            compiler_params=pltpu.CompilerParams(
                collective_id=0, has_side_effects=True, vmem_limit_bytes=67043328),
        )(signal, cond_feats, w_now, w_past, w_cond, b_gate, w_res, w_skip)

    seq = P('dp', 'sp', None)
    return jax.shard_map(local, mesh=mesh, in_specs=(seq, seq, P(), P(), P(), P(), P(), P()),
                         out_specs=(seq, seq), check_vma=False)
```

```python
import functools

import jax
import jax.numpy as jnp
from jax import lax
from jax.experimental import pallas as pl
from jax.experimental.pallas import tpu as pltpu
from jax.sharding import PartitionSpec as P

LAYERS = 10
NEAR = 5
RING = 8
BLOCKS = 16
CHUNKS = 4
SPAN = 32
ROWS = BLOCKS * SPAN
HALF = ROWS // 2
PAD = 2 * SPAN
RELAYED = 7
STRAIGHT = 3
WORD_BASE = 128
WORD_STEPS = 4
ORDER = (
    16794112, 4343301, 42156816, 101056913, 15141514, 52954932, 23878674, 84250276,
    135091772, 142855457, 78093490, 113985961, 71688381, 80645573, 130864938, 116494274,
    132896167, 268428227)
CH = 512
COND = 256
SKIP = 256
MESH = pl.DeviceIdType.MESH


def kernel(sig, cond, w_now, w_past, w_cond, bias, w_res, w_skip, h_out, s_out,
           wz, wr, ws, h, skip, cnd, ub, far, relay, shifted, edge_out, edge_in,
           w_sem, own_sem, in_send, in_recv, edge_send, edge_recv, far_send, far_recv, relay_send, relay_recv, out_send, out_recv, out_own):
    me = lax.axis_index('sp')
    row, lane = me // RING, lax.rem(me, RING)

    def ring(step):
        return {'sp': row * RING + lax.rem(lane + step, RING)}

    def peer(step):
        return lax.rem(row + step, BLOCKS)

    def hop(k):
        return 1 if k <= NEAR else 2 ** (k - NEAR)

    def weight_copies(k):
        return [pltpu.make_async_copy(w_now.at[k], wz.at[k, pl.ds(0, CH)], w_sem.at[k, 0]),
                pltpu.make_async_copy(w_past.at[k], wz.at[k, pl.ds(CH, CH)], w_sem.at[k, 1]),
                pltpu.make_async_copy(w_cond.at[k], wz.at[k, pl.ds(2 * CH, COND)], w_sem.at[k, 2]),
                pltpu.make_async_copy(w_res.at[k], wr.at[k], w_sem.at[k, 3]),
                pltpu.make_async_copy(w_skip.at[k], ws.at[k], w_sem.at[k, 4])]

    def block(b, start=0):
        return pl.ds(pl.multiple_of(start + b * SPAN, SPAN), SPAN)

    def own_inputs(c):
        seq = row * CHUNKS + c
        return [pltpu.make_async_copy(sig.at[seq], ub.at[0, c, block(row, PAD)], own_sem.at[c, 0]),
                pltpu.make_async_copy(cond.at[seq], cnd.at[c, block(row)], own_sem.at[c, 1])]

    def peer_inputs(c, step):
        to = peer(step)
        seq = to * CHUNKS + c
        dev = {'sp': to * RING + lane}
        return [pltpu.make_async_remote_copy(sig.at[seq], ub.at[0, c, block(row, PAD)], in_send.at[c, 0],
                                             in_recv.at[c, 0], device_id=dev, device_id_type=MESH),
                pltpu.make_async_remote_copy(cond.at[seq], cnd.at[c, block(row)], in_send.at[c, 1],
                                             in_recv.at[c, 1], device_id=dev, device_id_type=MESH)]

    def all_inputs(c):
        others = pl.ds(0, ROWS - SPAN)
        return [pltpu.make_async_remote_copy(ub.at[0, c, others], ub.at[0, c, others], in_send.at[c, 0],
                                             in_recv.at[c, 0], device_id=ring(1), device_id_type=MESH),
                pltpu.make_async_remote_copy(cnd.at[c, others], cnd.at[c, others], in_send.at[c, 1],
                                             in_recv.at[c, 1], device_id=ring(1), device_id_type=MESH)]

    def own_outputs(c):
        seq = row * CHUNKS + c
        return [pltpu.make_async_copy(h.at[c, block(row)], h_out.at[seq], out_own.at[c, 0]),
                pltpu.make_async_copy(skip.at[c, block(row)], s_out.at[seq], out_own.at[c, 1])]

    def peer_outputs(c, to):
        seq = row * CHUNKS + c
        dev = {'sp': to * RING + lane}
        return [pltpu.make_async_remote_copy(h.at[c, block(to)], h_out.at[seq], out_send.at[c, 0],
                                             out_recv.at[c, 0], device_id=dev, device_id_type=MESH),
                pltpu.make_async_remote_copy(skip.at[c, block(to)], s_out.at[seq], out_send.at[c, 1],
                                             out_recv.at[c, 1], device_id=dev, device_id_type=MESH)]

    def all_outputs(c):
        others = pl.ds(0, BLOCKS - 1)
        return [pltpu.make_async_remote_copy(h_out.at[others], h_out.at[others], out_send.at[c, 0],
                                             out_recv.at[c, 0], device_id=ring(1), device_id_type=MESH),
                pltpu.make_async_remote_copy(s_out.at[others], s_out.at[others], out_send.at[c, 1],
                                             out_recv.at[c, 1], device_id=ring(1), device_id_type=MESH)]

    def edge_copy(k, c):
        rows = pl.ds(BLOCKS * (2 ** k - 1), BLOCKS * 2 ** k)
        return pltpu.make_async_remote_copy(edge_out.at[c, rows], edge_in.at[c, rows], edge_send.at[k, c],
                                            edge_recv.at[k, c], device_id=ring(1), device_id_type=MESH)

    def far_copy(k, c, half, src=None, to=None):
        if src is None:
            src = ub.at[k % 2, c, pl.ds(PAD + half * HALF, HALF)]
        return pltpu.make_async_remote_copy(
            src, far.at[k - NEAR, c, pl.ds(SPAN + half * HALF, HALF)], far_send.at[k - NEAR, c, half],
            far_recv.at[k - NEAR, c, half], device_id=ring(hop(k) if to is None else to), device_id_type=MESH)

    def forward_copy(c, half):
        return far_copy(RELAYED, c, half, relay.at[c, pl.ds(half * HALF, HALF)], RING - 2)

    def relay_copy(c, half):
        return pltpu.make_async_remote_copy(
            ub.at[RELAYED % 2, c, pl.ds(PAD + half * HALF, HALF)], relay.at[c, pl.ds(half * HALF, HALF)],
            relay_send.at[c, half], relay_recv.at[c, half], device_id=ring(RING - 2), device_id_type=MESH)

    def on_route(c, relayed, straight):
        @pl.when(c < STRAIGHT)
        def _():
            relayed()

        @pl.when(c >= STRAIGHT)
        def _():
            straight()

    def send_far(k, c, half):
        if k == RELAYED:
            on_route(c, relay_copy(c, half).start, far_copy(k, c, half).start)
        else:
            far_copy(k, c, half).start()

    def wait_sent(k, c, half):
        if k == RELAYED:
            on_route(c, relay_copy(c, half).wait_send, far_copy(k, c, half).wait_send)
        else:
            far_copy(k, c, half).wait_send()

    for c in range(CHUNKS):
        for copy in own_inputs(c):
            copy.start()
    for copy in weight_copies(0):
        copy.start()

    barrier = pltpu.get_barrier_semaphore()
    ring_steps = (1, 2, 4, RING - 2, RING - 1)
    for step in ring_steps:
        pl.semaphore_signal(barrier, inc=1, device_id=ring(step), device_id_type=MESH)
    for step in range(1, BLOCKS):
        pl.semaphore_signal(barrier, inc=1, device_id={'sp': peer(step) * RING + lane}, device_id_type=MESH)
    pl.semaphore_wait(barrier, len(ring_steps) + BLOCKS - 1)

    def start_inputs(i, carry):
        c, step = i // (BLOCKS - 1), lax.rem(i, BLOCKS - 1) + 1
        for copy in peer_inputs(c, step):
            copy.start()
        return carry

    lax.fori_loop(0, CHUNKS * (BLOCKS - 1), start_inputs, 0)
    for k in range(1, LAYERS):
        for copy in weight_copies(k):
            copy.start()

    for c in range(CHUNKS):
        for parity in range(2):
            ub[parity, c, pl.ds(0, PAD)] = jnp.zeros((PAD, CH), jnp.bfloat16)
        for k in range(far.shape[0]):
            far[k, c, pl.ds(0, SPAN)] = jnp.zeros((SPAN, CH), jnp.bfloat16)

    lanes = range(CH // 128)

    def send_edges(k, c):
        d = 2 ** k

        def roll(b, carry):
            for t in lanes:
                shifted[c, t, block(b)] = pltpu.roll(h[c, block(b), pl.ds(128 * t, 128)], d, 0)
            return carry

        lax.fori_loop(0, BLOCKS, roll, 0)
        for j in range(d):
            for t in lanes:
                rows = shifted[c, t, pl.ds(j, BLOCKS, stride=SPAN), :]
                edge_out[c, pl.ds(BLOCKS * (d - 1 + j), BLOCKS), pl.ds(128 * t, 128)] = rows.astype(jnp.bfloat16)
        edge_copy(k, c).start()

    def arrive(c):
        for copy in own_inputs(c):
            copy.wait()
        for copy in all_inputs(c):
            copy.wait_recv()
        h[c] = ub[0, c, pl.ds(PAD, ROWS)].astype(jnp.float32)
        send_edges(0, c)

    def receive_edges(k, c):
        d = 2 ** k
        edge_copy(k, c).wait_recv()

        def patch(start):
            for j in range(d):
                for t in lanes:
                    rows = edge_in[c, pl.ds(BLOCKS * (d - 1 + j), BLOCKS), pl.ds(128 * t, 128)]
                    shifted[c, t, pl.ds(start + j, BLOCKS, stride=SPAN), :] = rows.astype(jnp.float32)

        @pl.when(lane > 0)
        def _():
            patch(0)

        @pl.when(lane == 0)
        def _():
            patch(SPAN)
            for t in lanes:
                shifted[c, t, pl.ds(0, d)] = jnp.zeros((d, 128), jnp.float32)

    def compute(k, c, first, count):
        rows = pl.ds(first, count)
        own = ub[k % 2, c, pl.ds(PAD + first, count)]
        if k < NEAR:
            past = jnp.concatenate([shifted[c, t, rows].astype(jnp.bfloat16) for t in lanes], axis=1)
        elif k < far.shape[0] + NEAR:
            wrapped = (lane < hop(k)).astype(jnp.int32)
            start = pl.multiple_of(SPAN - SPAN * wrapped + first, SPAN)
            past = far[k - NEAR, c, pl.ds(start, count)]
        else:
            past = ub[k % 2, c, pl.ds(PAD - SPAN * (k - RELAYED) + first, count)]
        x = jnp.concatenate([own, past, cnd[c, rows]], axis=1)
        gated = []
        for col in range(0, CH, 256):
            zf = jnp.dot(x, wz[k, :, col:col + 256], preferred_element_type=jnp.float32)
            zg = jnp.dot(x, wz[k, :, CH + col:CH + col + 256], preferred_element_type=jnp.float32)
            zf = zf + bias[k:k + 1, col:col + 256]
            zg = zg + bias[k:k + 1, CH + col:CH + col + 256]
            gated.append((jnp.tanh(zf) * (0.5 * jnp.tanh(0.5 * zg) + 0.5)).astype(jnp.bfloat16))
        a = jnp.concatenate(gated, axis=1)
        for col in range(0, CH, 256):
            cols = pl.ds(col, 256)
            new = h[c, rows, cols] + jnp.dot(a, wr[k, :, col:col + 256], preferred_element_type=jnp.float32)
            h[c, rows, cols] = new
            if k + 1 < LAYERS:
                ub[(k + 1) % 2, c, pl.ds(PAD + first, count), cols] = new.astype(jnp.bfloat16)
        add = jnp.dot(a, ws[k], preferred_element_type=jnp.float32)
        skip[c, rows] = add if k == 0 else skip[c, rows] + add

    def near_layer(k, c):
        @pl.when(c == 0)
        def _():
            for copy in weight_copies(k):
                copy.wait()

        receive_edges(k, c)
        compute(k, c, 0, ROWS)
        if k + 1 < NEAR:
            send_edges(k + 1, c)
        else:
            for half in range(2):
                send_far(NEAR, c, half)

    def far_layer(k, half, c):
        if half == 0:
            @pl.when(c == 0)
            def _():
                for copy in weight_copies(k):
                    copy.wait()

        if k <= RELAYED:
            far_copy(k, c, half).wait_recv()
        if NEAR <= k - 1 <= RELAYED:
            wait_sent(k - 1, c, half)
        compute(k, c, half * HALF, HALF)
        if k < RELAYED:
            send_far(k + 1, c, half)
        if k + 1 == LAYERS:
            blocks = BLOCKS // 2

            @pl.when(row // blocks == half)
            def _():
                for copy in own_outputs(c):
                    copy.start()

            def start_outputs(i, carry):
                to = half * blocks + lax.rem(row + i, blocks)

                @pl.when(to != row)
                def _():
                    for copy in peer_outputs(c, to):
                        copy.start()
                return carry

            lax.fori_loop(0, blocks, start_outputs, 0)

    def forward(half, c):
        relay_copy(c, half).wait_recv()
        forward_copy(c, half).start()

    steps = [arrive] + [functools.partial(near_layer, k) for k in range(NEAR)]
    for half in range(2):
        steps += [functools.partial(far_layer, k, half) for k in range(NEAR, RELAYED)]
        steps += [functools.partial(forward, half)]
        steps += [functools.partial(far_layer, k, half) for k in range(RELAYED, LAYERS)]

    def run_word(i, carry):
        word = sum(jnp.where(i == j, packed, 0) for j, packed in enumerate(ORDER))

        def run_step(_, word):
            step, c = lax.div(lax.rem(word, WORD_BASE), CHUNKS), lax.rem(word, CHUNKS)
            for start in range(0, len(steps), 5):
                @pl.when((step >= start) & (step < start + 5))
                def _(start=start):
                    for index in range(start, min(start + 5, len(steps))):
                        @pl.when(step == index)
                        def _(index=index):
                            steps[index](c)
            return lax.div(word, WORD_BASE)

        lax.fori_loop(0, WORD_STEPS, run_step, word)
        return carry

    lax.fori_loop(0, len(ORDER), run_word, 0)

    def finish(c, carry):
        for copy in all_inputs(c):
            copy.wait_send()
        for k in range(NEAR):
            edge_copy(k, c).wait_send()
        @pl.when(c < STRAIGHT)
        def _():
            for half in range(2):
                forward_copy(c, half).wait_send()

        for copy in own_outputs(c):
            copy.wait()
        for copy in all_outputs(c):
            copy.wait_send()
            copy.wait_recv()
        return carry

    lax.fori_loop(0, CHUNKS, finish, 0)


def solution(mesh):
    def local(signal, cond_feats, w_now, w_past, w_cond, b_gate, w_res, w_skip):
        hbm = pl.BlockSpec(memory_space=pl.ANY)
        dma = pltpu.SemaphoreType.DMA
        return pl.pallas_call(
            kernel,
            out_shape=(jax.ShapeDtypeStruct(signal.shape, jnp.float32),
                       jax.ShapeDtypeStruct(signal.shape[:2] + (SKIP,), jnp.float32)),
            in_specs=[hbm] * 5 + [pl.BlockSpec(memory_space=pltpu.VMEM)] + [hbm] * 2,
            out_specs=(hbm, hbm),
            scratch_shapes=[
                pltpu.VMEM((LAYERS, 2 * CH + COND, 2 * CH), jnp.bfloat16),
                pltpu.VMEM((LAYERS, CH, CH), jnp.bfloat16),
                pltpu.VMEM((LAYERS, CH, SKIP), jnp.bfloat16),
                pltpu.VMEM((CHUNKS, ROWS, CH), jnp.float32),
                pltpu.VMEM((CHUNKS, ROWS, SKIP), jnp.float32),
                pltpu.VMEM((CHUNKS, ROWS, COND), jnp.bfloat16),
                pltpu.VMEM((2, CHUNKS, PAD + ROWS, CH), jnp.bfloat16),
                pltpu.VMEM((3, CHUNKS, SPAN + ROWS, CH), jnp.bfloat16),
                pltpu.VMEM((CHUNKS, ROWS, CH), jnp.bfloat16),
                pltpu.VMEM((CHUNKS, CH // 128, SPAN + ROWS, 128), jnp.float32),
                pltpu.VMEM((CHUNKS, BLOCKS * (SPAN - 1), CH), jnp.bfloat16),
                pltpu.VMEM((CHUNKS, BLOCKS * (SPAN - 1), CH), jnp.bfloat16),
                dma((LAYERS, 5)), dma((CHUNKS, 2)), dma((CHUNKS, 2)), dma((CHUNKS, 2)),
                dma((NEAR, CHUNKS)), dma((NEAR, CHUNKS)), dma((3, CHUNKS, 2)), dma((3, CHUNKS, 2)),
                dma((CHUNKS, 2)), dma((CHUNKS, 2)),
                dma((CHUNKS, 2)), dma((CHUNKS, 2)), dma((CHUNKS, 2)),
            ],
            compiler_params=pltpu.CompilerParams(
                collective_id=0, has_side_effects=True, vmem_limit_bytes=67043328),
        )(signal, cond_feats, w_now, w_past, w_cond, b_gate, w_res, w_skip)

    seq = P('dp', 'sp', None)
    return jax.shard_map(local, mesh=mesh, in_specs=(seq, seq, P(), P(), P(), P(), P(), P()),
                         out_specs=(seq, seq), check_vma=False)
```
